128 devices in a mesh: row: 32 (over z, x, core), sub: 4 (over y).
Axes of the slice: x: 4, y: 4, z: 4, core: 2. Of those that a mesh axis runs over, the one named last changes fastest.
Arguments:
- eig_vectors: float32 [262144, 512], P(('row', 'sub')), may hold values from -0.01171875 to 0.01171875
- vec_cotangent: float32 [262144, 512], P(('row', 'sub')), may hold values from -3072 to 3072
- levels: float32 [512], replicated, may hold values from -2 to 2
- order: int32 [512], replicated, may hold values from 0 to 511, each once
- neighbours: int32 [2048, 12], P(('row', 'sub')), may hold values from 0 to 2047, as said below
Outputs:
- grad_blocks: float32 [2048, 12, 128, 128], P(('row', 'sub'))
The draws below stay inside these ranges and needn't reach their ends.
Inputs may be any that keep to these rules, and one draw needn't show every extreme that they name: `neighbours`: entry 0 of row i is i itself. Row blocks are dealt to devices in order, 16 to a device, device index = row index * 4 + sub index; every listed block lies on the row block's own device or on a device whose row index or sub index (not both) differs by one, cyclically.
All inputs are finite; a program needn't handle non-finite values.
Results may differ from the reference program's by a relative error of at most 0.0003.
Values sent between devices are 32-bit elements; how exact they have to be, the bound alone decides.
No kernel may reach another device: no remote copies, remote signals or barrier semaphores. Data moves between devices by JAX's collectives and lax.ppermute only.
A program may use at most 192 MiB of HBM per device.

```python
import jax
import jax.numpy as jnp
from jax import lax

WINDOW = 512
BS = 128
NNBR = 12
BLK_DEV = 16
DEV_ROW = 32
DEV_SUB = 4
NBLK = 2048
NROWS = 262144


def draw_neighbours(key, part):
    key_dir = jax.random.fold_in(key, 11)
    key_loc = jax.random.fold_in(key, 12)
    blocks = jnp.arange(NBLK, dtype=jnp.int32)
    device = blocks // BLK_DEV
    row_pos = device // DEV_SUB
    sub_pos = device % DEV_SUB
    direction = jax.random.randint(key_dir, (NBLK, NNBR), 0, 5, dtype=jnp.int32)
    local = jax.random.randint(key_loc, (NBLK, NNBR), 0, BLK_DEV, dtype=jnp.int32)
    row_step = jnp.where(direction == 1, 1, jnp.where(direction == 2, -1, 0))
    sub_step = jnp.where(direction == 3, 1, jnp.where(direction == 4, -1, 0))
    row_new = (row_pos[:, None] + row_step + DEV_ROW) % DEV_ROW
    sub_new = (sub_pos[:, None] + sub_step + DEV_SUB) % DEV_SUB
    listed = (row_new * DEV_SUB + sub_new) * BLK_DEV + local
    listed = listed.at[:, 0].set(blocks)
    return listed.astype(jnp.int32)


def level_of(key, dims, shards, low, top_value):
    def one(axis_at, blocks):
        steps = jax.random.uniform(jax.random.fold_in(jax.random.fold_in(key, 6), axis_at), (blocks,), jnp.float32, low / len(shards), top_value / len(shards))
        return jnp.repeat(jnp.exp(steps), dims[axis_at] // blocks).reshape((-1,) + (1,) * (len(dims) - axis_at - 1))

    factor_of = one(*shards[0])
    for cut in shards[1:]:
        factor_of = factor_of * one(*cut)
    return factor_of


def gaussian(key, dims, width, reach, shards=(), kind=jnp.bfloat16):
    gain = level_of(key, dims, shards, -0.22, 0.18) if shards else 1.0
    result = jax.random.normal(key, dims, jnp.float32) * width * gain
    return jnp.minimum(jnp.maximum(result, -reach), reach).astype(kind)


def setup_inputs(seed: int = 0) -> dict:
    keys = jax.random.split(jax.random.key(seed), 6)
    eig_vectors = gaussian(keys[0], (NROWS, WINDOW), NROWS ** -0.5, 0.01171875, ((0, 128),), jnp.float32)
    vec_cotangent = gaussian(keys[1], (NROWS, WINDOW), (NROWS // WINDOW), 3072.0, ((0, 128),), jnp.float32)
    levels = jnp.clip(jax.random.uniform(keys[2], (WINDOW,), jnp.float32, -2.0, 2.0), -2.0, 2.0)
    order = jax.random.permutation(keys[3], WINDOW).astype(jnp.int32)
    neighbours = draw_neighbours(jax.random.fold_in(keys[5], 71), 0)
    return dict(eig_vectors=eig_vectors, vec_cotangent=vec_cotangent, levels=levels, order=order, neighbours=neighbours)


broadening_sq = 0.0025


def reference(eig_vectors, vec_cotangent, levels, order, neighbours):
    highest = lax.Precision.HIGHEST
    energy = levels[order.astype(jnp.int32)]
    spread = energy[None, :] - energy[:, None]
    gap_factor = spread / (spread * spread + broadening_sq)
    gram = lax.dot_general(eig_vectors, vec_cotangent, (((0,), (0,)), ((), ())), precision=highest, preferred_element_type=jnp.float32)
    scaled = gap_factor * gram
    adjoint_rows = jnp.dot(eig_vectors, scaled, precision=highest, preferred_element_type=jnp.float32)
    window = eig_vectors.shape[1]
    vec_blocks = eig_vectors.reshape(NBLK, BS, window)
    adj_blocks = adjoint_rows.reshape(NBLK, BS, window)

    def one_block(inputs_pair):
        adj_block, listed = inputs_pair
        picked = vec_blocks[listed.astype(jnp.int32)]
        return jnp.einsum("ak,nbk->nab", adj_block, picked, precision=highest)

    return lax.map(one_block, (adj_blocks, neighbours))
```

```python
import functools

import jax
import jax.numpy as jnp
from jax import lax
from jax.experimental import pallas as pl
from jax.experimental.pallas import tpu as pltpu
from jax.sharding import PartitionSpec as P


BS = 128
broadening_sq = 0.0025

N_CORE, N_X, N_Z = 2, 4, 4
N_ROW, N_SUB = N_CORE * N_X * N_Z, 4

PIECES = (6, 7, 3)
STAGES, UNROLL, FETCH, STEP = 8, 8, 6, 4
WHOLE_VMEM = 62 * 2**20
SELF, NEAR, FAR, SUB_LOW, SUB_HIGH = range(5)


def row_shift(dz, dx):
    pairs = []
    for r in range(N_ROW):
        core, x, z = r % N_CORE, (r // N_CORE) % N_X, r // (N_CORE * N_X)
        target = (((z + dz) % N_Z) * N_X + (x + dx) % N_X) * N_CORE + core
        pairs.append((r, target))
    return pairs


CORE_SWAP = [(r, r ^ 1) for r in range(N_ROW)]


PASS_ON = [(r, (r + (-2 if r % 2 else 2)) % N_ROW) for r in range(N_ROW)]


def ring(count, step):
    return [(i, (i + step) % count) for i in range(count)]


def part(array, index, size):
    return lax.dynamic_slice_in_dim(array, index * size, size, axis=0)


def gather_back(mine, count, send):
    return jnp.concatenate([mine] + [send(step) for step in range(1, count)])


def split(value):
    high = value.astype(jnp.bfloat16)
    return high, (value - high.astype(jnp.float32)).astype(jnp.bfloat16)


def turn_kernel(blocks, out, held, turned, sems, out_sems):
    count = out.shape[0]
    fetch = [pltpu.make_async_copy(blocks.at[b], held.at[b], sems.at[b]) for b in range(count)]
    store = [pltpu.make_async_copy(turned.at[b], out.at[b], out_sems.at[b]) for b in range(count)]
    for b in range(count):
        fetch[b].start()
    for b in range(count):
        fetch[b].wait()
        turned[b] = held[b].T
        store[b].start()
    for b in range(count):
        store[b].wait()


def turn(blocks, count):
    _, rows, window = blocks.shape
    return pl.pallas_call(
        turn_kernel,
        out_shape=jax.ShapeDtypeStruct((count, window, rows), jnp.float32),
        in_specs=[pl.BlockSpec(memory_space=pltpu.HBM)],
        out_specs=pl.BlockSpec(memory_space=pltpu.HBM),
        scratch_shapes=[
            pltpu.VMEM((count, rows, window), jnp.float32),
            pltpu.VMEM((count, window, rows), jnp.float32),
            pltpu.SemaphoreType.DMA((count,)),
            pltpu.SemaphoreType.DMA((count,)),
        ],
        compiler_params=pltpu.CompilerParams(vmem_limit_bytes=WHOLE_VMEM),
        cost_estimate=pl.CostEstimate(
            flops=10**9, bytes_accessed=2 * count * rows * window * 4, transcendentals=0
        ),
        name="turn",
    )(blocks)


def front_kernel(spans, blocks, other, *refs):
    n_out = len(spans)
    outs = refs[:n_out]
    divided, gram, q, v, turned, halves, q_sems, v_sems, t_sems, d_sems = refs[n_out:]
    count = blocks.shape[0]

    def fetch(b):
        return (
            pltpu.make_async_copy(blocks.at[b], q.at[b], q_sems.at[b]),
            pltpu.make_async_copy(other.at[b], v.at[b], v_sems.at[b]),
        )

    def keep(b):
        return pltpu.make_async_copy(halves.at[b], divided.at[b], d_sems.at[b])

    def store(b, low, out):
        return pltpu.make_async_copy(turned.at[b], out.at[b - low], t_sems.at[b])

    for b in range(count):
        for copy in fetch(b):
            copy.start()
    gram[...] = jnp.zeros_like(gram)

    def step(n, _):
        left, right = [], []
        for u in range(STEP):
            b = n * STEP + u
            for copy in fetch(b):
                copy.wait()
            t = q[b].T
            turned[b] = t
            high, low = split(t)
            halves[b, :, :BS] = high
            halves[b, :, BS:] = low
            keep(b).start()
            for (first, last), out in zip(spans, outs):

                @pl.when((b >= first) & (b < last))
                def _(first=first, out=out):
                    store(b, first, out).start()

            vh, vl = split(v[b])
            left += [high, high, low]
            right += [vh, vl, vh]
        gram[...] += jnp.dot(
            jnp.concatenate(left, axis=1),
            jnp.concatenate(right, axis=0),
            preferred_element_type=jnp.float32,
        )
        return 0

    lax.fori_loop(0, count // STEP, step, 0)
    for b in range(count):
        keep(b).wait()
        for (first, last), out in zip(spans, outs):
            if first <= b < last:
                store(b, first, out).wait()


def front(blocks, other, spans):
    count, rows, window = blocks.shape
    hbm = pl.BlockSpec(memory_space=pltpu.HBM)
    return pl.pallas_call(
        functools.partial(front_kernel, spans),
        out_shape=[
            jax.ShapeDtypeStruct((high - low, window, rows), jnp.float32) for low, high in spans
        ]
        + [
            jax.ShapeDtypeStruct((count, window, 2 * rows), jnp.bfloat16),
            jax.ShapeDtypeStruct((window, window), jnp.float32),
        ],
        in_specs=[hbm, hbm],
        out_specs=[hbm] * (len(spans) + 1) + [pl.BlockSpec(memory_space=pltpu.VMEM)],
        scratch_shapes=[
            pltpu.VMEM((count, rows, window), jnp.float32),
            pltpu.VMEM((count, rows, window), jnp.float32),
            pltpu.VMEM((count, window, rows), jnp.float32),
            pltpu.VMEM((count, window, 2 * rows), jnp.bfloat16),
        ]
        + [pltpu.SemaphoreType.DMA((count,))] * 4,
        compiler_params=pltpu.CompilerParams(vmem_limit_bytes=WHOLE_VMEM),
        cost_estimate=pl.CostEstimate(
            flops=6 * count * rows * window * window, bytes_accessed=2**24, transcendentals=0
        ),
        name="front",
    )(blocks, other)


def adjoint_kernel(place, blocks, mine, other, factor, out, q, sh, sl, sems):
    count = blocks.shape[0]
    half = mine.shape[0]
    copies = [pltpu.make_async_copy(blocks.at[b], q.at[b], sems.at[b]) for b in range(count)]
    for copy in copies:
        copy.start()
    core, x, z = place[0], place[1], place[2]
    size = half // (N_X * N_Z)
    for index, ref in enumerate((mine, other)):
        start = jnp.where(core == index, 0, half)
        for i in range(N_X):
            for j in range(N_Z):
                at = start + (lax.rem(x + N_X - i, N_X) * N_Z + lax.rem(z + N_Z - j, N_Z)) * size
                rows = pl.ds(pl.multiple_of(at, size), size)
                part_of = ref[(i * N_Z + j) * size : (i * N_Z + j + 1) * size, :]
                sh[rows, :], sl[rows, :] = split(factor[rows, :] * part_of)

    def some(n, _):
        for u in range(STEP):
            i = n * STEP + u
            pltpu.make_async_copy(blocks.at[i], q.at[i], sems.at[i]).wait()
            qh, ql = split(q[i])
            both = jnp.concatenate([qh, ql], axis=0)
            first = jnp.dot(both, sh[...], preferred_element_type=jnp.float32)
            second = jnp.dot(qh, sl[...], preferred_element_type=jnp.float32)
            high, low = split(first[:BS] + (first[BS:] + second))
            out[i, :BS, :] = high
            out[i, BS:, :] = low
        return 0

    lax.fori_loop(0, count // STEP, some, 0)


def adjoint(place, blocks, mine, other, factor):
    count, rows, window = blocks.shape
    vmem = pl.BlockSpec(memory_space=pltpu.VMEM)
    return pl.pallas_call(
        adjoint_kernel,
        out_shape=jax.ShapeDtypeStruct((count, 2 * rows, window), jnp.bfloat16),
        in_specs=[pl.BlockSpec(memory_space=pltpu.SMEM), pl.BlockSpec(memory_space=pltpu.HBM)]
        + [vmem] * 3,
        out_specs=vmem,
        scratch_shapes=[
            pltpu.VMEM((count, rows, window), jnp.float32),
            pltpu.VMEM((window, window), jnp.bfloat16),
            pltpu.VMEM((window, window), jnp.bfloat16),
            pltpu.SemaphoreType.DMA((count,)),
        ],
        compiler_params=pltpu.CompilerParams(vmem_limit_bytes=WHOLE_VMEM),
        cost_estimate=pl.CostEstimate(
            flops=6 * count * rows * window * window, bytes_accessed=2**23, transcendentals=0
        ),
        name="adjoint",
    )(place, blocks, mine, other, factor)


def pair_kernel(counts, own, group, bounds, keys, adjoint_blocks, *refs):
    n_src = len(counts)
    sources = refs[:n_src]
    out, held, adjoints, fetched, stage, sems, fetch_sems, own_sem, adjoint_sem = refs[-9:]
    base = own
    pieces = [(source, b) for source, count in zip(sources, counts) for b in range(count)]
    copies = [
        pltpu.make_async_copy(source.at[b], fetched.at[n % FETCH], fetch_sems.at[n % FETCH])
        for n, (source, b) in enumerate(pieces)
    ]
    for copy in copies[:FETCH]:
        copy.start()
    adjoint_copy = pltpu.make_async_copy(adjoint_blocks, adjoints, adjoint_sem)
    adjoint_copy.start()
    if own:
        own_copy = pltpu.make_async_copy(refs[n_src], held.at[pl.ds(0, own)], own_sem)
        own_copy.start()
    for n, copy in enumerate(copies):
        copy.wait()
        high, low = split(fetched[n % FETCH])
        held[base + n, :, :BS] = high
        held[base + n, :, BS:] = low
        if n + FETCH < len(copies):
            copies[n + FETCH].start()
    adjoint_copy.wait()
    if own:
        own_copy.wait()
    first, last = bounds[group], bounds[group + 1]
    origin = bounds[group + 8]
    total = last - first

    def copy_out(slot, target):
        return pltpu.make_async_copy(stage.at[slot], out.at[target], sems.at[slot])

    def some(step, _):
        products, targets = [], []
        for u in range(UNROLL):
            key = keys[jnp.minimum(first + step * UNROLL + u, last - 1)]
            b, i, k = (key >> 8) - origin, (key >> 4) & 15, key & 15
            product = jnp.dot(adjoints[i], held[b], preferred_element_type=jnp.float32)
            products.append(
                product[:BS, :BS]
                + ((product[:BS, BS:] + product[BS:, :BS]) + product[BS:, BS:])
            )
            targets.append(i * 12 + k)
        for u in range(UNROLL):
            at = step * UNROLL + u
            slot = lax.rem(at, STAGES)

            @pl.when((at >= STAGES) & (at - STAGES < total))
            def _():
                copy_out(slot, 0).wait()

            stage[slot] = products[u]

            @pl.when(at < total)
            def _():
                copy_out(slot, targets[u]).start()

        return 0

    steps = lax.div(total + (UNROLL - 1), UNROLL)
    lax.fori_loop(0, steps, some, 0)
    done = steps * UNROLL
    for s in range(STAGES):
        at = done - STAGES + s

        @pl.when((at >= 0) & (at < total))
        def _():
            copy_out(lax.rem(at, STAGES), 0).wait()


def pair_call(group, bounds, keys, adjoints, sources, own, out, shape):
    counts = tuple(s.shape[0] for s in sources)
    n_own = 0 if own is None else own.shape[0]
    n_blk = sum(counts) + n_own
    smem = pl.BlockSpec(memory_space=pltpu.SMEM)
    hbm = pl.BlockSpec(memory_space=pltpu.HBM)
    window = adjoints.shape[-1]
    operands = [bounds, keys, adjoints, *sources]
    if own is not None:
        operands.append(own)
    aliases = {}
    if out is not None:
        aliases = {len(operands): 0}
        operands.append(out)
    return pl.pallas_call(
        functools.partial(pair_kernel, counts, n_own, group),
        out_shape=jax.ShapeDtypeStruct(shape, jnp.float32),
        in_specs=[smem, smem] + [hbm] * (len(operands) - 2),
        out_specs=hbm,
        scratch_shapes=[
            pltpu.VMEM((n_blk, window, 2 * BS), jnp.bfloat16),
            pltpu.VMEM(adjoints.shape, jnp.bfloat16),
            pltpu.VMEM((FETCH, window, BS), jnp.float32),
            pltpu.VMEM((STAGES, BS, BS), jnp.float32),
            pltpu.SemaphoreType.DMA((STAGES,)),
            pltpu.SemaphoreType.DMA((FETCH,)),
            pltpu.SemaphoreType.DMA,
            pltpu.SemaphoreType.DMA,
        ],
        input_output_aliases=aliases,
        compiler_params=pltpu.CompilerParams(vmem_limit_bytes=WHOLE_VMEM),
        cost_estimate=pl.CostEstimate(
            flops=n_blk * 4 * 2 * BS * BS * window, bytes_accessed=8 * 2**20, transcendentals=0
        ),
    )(*operands)


def body(eig_vectors, vec_cotangent, levels, order, neighbours):
    highest = lax.Precision.HIGHEST
    window = eig_vectors.shape[1]
    local_rows = eig_vectors.shape[0]
    blk_count = local_rows // BS
    n_nbr = neighbours.shape[1]
    my_row, my_sub = lax.axis_index("row"), lax.axis_index("sub")
    core, x, z = my_row % N_CORE, (my_row // N_CORE) % N_X, my_row // (N_CORE * N_X)
    blocks = eig_vectors.reshape(blk_count, BS, window)

    spans = [(sum(PIECES[:n]), sum(PIECES[: n + 1])) for n in range(len(PIECES))]
    turned = [turn(blocks, PIECES[0])]
    *rest, divided, partial_gram = front(
        blocks, vec_cotangent.reshape(blk_count, BS, window), spans[1:]
    )
    turned += rest
    sub_low = [lax.ppermute(t, "sub", ring(N_SUB, 1)) for t in turned]
    sub_high = [lax.ppermute(t, "sub", ring(N_SUB, -1)) for t in turned]
    near = [lax.ppermute(t, "row", CORE_SWAP) for t in turned]
    far = [lax.ppermute(t, "row", PASS_ON) for t in near]

    half = window // N_CORE
    total = part(partial_gram, core, half) + lax.ppermute(
        part(partial_gram, 1 - core, half), "row", CORE_SWAP
    )
    quarter = half // N_X
    mine = part(total, x, quarter)
    for s in range(1, N_X):
        mine += lax.ppermute(part(total, (x + s) % N_X, quarter), "row", row_shift(0, s))
    piece = quarter // N_Z
    total = mine
    mine = part(total, z, piece)
    for s in range(1, N_Z):
        mine += lax.ppermute(part(total, (z + s) % N_Z, piece), "row", row_shift(s, 0))
    total = mine
    for s in range(1, N_SUB):
        total += lax.ppermute(mine, "sub", ring(N_SUB, s))
    total = gather_back(total, N_Z, lambda s: lax.ppermute(total, "row", row_shift(s, 0)))
    total = gather_back(total, N_X, lambda s: lax.ppermute(total, "row", row_shift(0, s)))
    other = lax.ppermute(total, "row", CORE_SWAP)
    columns = lax.broadcasted_iota(jnp.int32, (window, window), 1)
    picked = (order[:, None] == columns).astype(jnp.float32)
    energy = jnp.dot(picked, levels, precision=highest, preferred_element_type=jnp.float32)
    spread = energy[None, :] - energy[:, None]
    factor = spread / (spread * spread + broadening_sq)
    place = jnp.stack([core, x, z]).astype(jnp.int32)

    device = neighbours // blk_count
    local = neighbours % blk_count
    row_delta = (device // N_SUB - my_row + N_ROW) % N_ROW
    sub_delta = (device % N_SUB - my_sub + N_SUB) % N_SUB
    slot = jnp.where(sub_delta == 1, SUB_HIGH, jnp.where(sub_delta == N_SUB - 1, SUB_LOW, SELF))
    slot = jnp.where(row_delta == jnp.where(core == 0, 1, N_ROW - 1), NEAR, slot)
    slot = jnp.where(row_delta == jnp.where(core == 0, N_ROW - 1, 1), FAR, slot)
    near = [(NEAR, low, array) for (low, _), array in zip(spans, near)]
    far = [(FAR, low, array) for (low, _), array in zip(spans, far)]
    sub = [
        [(SUB_LOW, low, below), (SUB_HIGH, low, above)]
        for (low, _), below, above in zip(spans, sub_low, sub_high)
    ]
    groups = [
        [(SELF, 0, divided)] + near + [far[0]] + sub[0],
        far[1:] + sub[1],
        sub[2],
    ]
    position = jnp.zeros_like(slot)
    base, origins = 0, []
    for group in groups:
        origins.append(base)
        for which, low, array in group:
            inside = (slot == which) & (local >= low) & (local < low + array.shape[0])
            position = jnp.where(inside, base + local - low, position)
            base += array.shape[0]
    i_index = lax.broadcasted_iota(jnp.int32, position.shape, 0)
    k_index = lax.broadcasted_iota(jnp.int32, position.shape, 1)
    key = (position * 256 + i_index * 16 + k_index).reshape(-1)
    rank = jnp.sum((key[:, None] > key[None, :]).astype(jnp.int32), axis=1)
    n_pair = key.shape[0]
    places = lax.broadcasted_iota(jnp.int32, (n_pair, n_pair), 0)
    keys = jnp.sum(jnp.where(rank[None, :] == places, key[None, :], 0), axis=1)
    limits = jnp.array(origins + [base] * (8 - len(origins)), jnp.int32)
    starts = jnp.sum((position.reshape(1, -1) < limits[:, None]).astype(jnp.int32), axis=1)
    bounds = jnp.concatenate([starts, limits])

    adjoints = adjoint(place, blocks, total, other, factor)
    out = None
    shape = (blk_count * n_nbr, BS, BS)
    for index, group in enumerate(groups):
        arrays = [g[2] for g in group]
        own = arrays.pop(0) if index == 0 else None
        out = pair_call(index, bounds, keys, adjoints, arrays, own, out, shape)
    return out.reshape(blk_count, n_nbr, BS, BS)


def solution(mesh):
    in_specs = (P(("row", "sub"), None), P(("row", "sub"), None), P(), P(), P(("row", "sub"), None))
    out_specs = P(("row", "sub"), None, None, None)
    return jax.shard_map(body, mesh=mesh, in_specs=in_specs, out_specs=out_specs, check_vma=False)
```

```python
import functools

import jax
import jax.numpy as jnp
from jax import lax
from jax.experimental import pallas as pl
from jax.experimental.pallas import tpu as pltpu
from jax.sharding import PartitionSpec as P


BS = 128
broadening_sq = 0.0025

N_CORE, N_X, N_Z = 2, 4, 4
N_ROW, N_SUB = N_CORE * N_X * N_Z, 4

SUB_PIECES = (6, 7, 3)
ROW_PIECES = (4, 6, 4, 2)
STAGES, UNROLL, STEP = 16, 8, 4
WHOLE_VMEM = 62 * 2**20
SELF, NEAR, FAR, SUB_LOW, SUB_HIGH = range(5)


def row_shift(dz, dx):
    pairs = []
    for r in range(N_ROW):
        core, x, z = r % N_CORE, (r // N_CORE) % N_X, r // (N_CORE * N_X)
        target = (((z + dz) % N_Z) * N_X + (x + dx) % N_X) * N_CORE + core
        pairs.append((r, target))
    return pairs


CORE_SWAP = [(r, r ^ 1) for r in range(N_ROW)]


PASS_ON = [(r, (r + (-2 if r % 2 else 2)) % N_ROW) for r in range(N_ROW)]


def ring(count, step):
    return [(i, (i + step) % count) for i in range(count)]


def part(array, index, size):
    return lax.dynamic_slice_in_dim(array, index * size, size, axis=0)


def gather_back(mine, count, send):
    return jnp.concatenate([mine] + [send(step) for step in range(1, count)])


def split(value):
    high = value.astype(jnp.bfloat16)
    return high, (value - high.astype(jnp.float32)).astype(jnp.bfloat16)


def turn_kernel(spans, blocks, *refs):
    n_out = len(spans)
    outs = refs[:n_out]
    q, turned, q_sems, t_sems = refs[n_out:]
    low = min(first for first, _ in spans)
    count = q.shape[0]

    def fetch(b):
        return pltpu.make_async_copy(blocks.at[low + b], q.at[b], q_sems.at[b])

    def store(n, b):
        at = low + b - spans[n][0]
        return pltpu.make_async_copy(turned.at[b], outs[n].at[at], t_sems.at[n, b])

    for b in range(count):
        fetch(b).start()

    def step(b, _):
        fetch(b).wait()
        turned[b] = q[b].T
        for n, (first, last) in enumerate(spans):

            @pl.when((low + b >= first) & (low + b < last))
            def _(n=n):
                store(n, b).start()

        return 0

    lax.fori_loop(0, count, step, 0)
    for n, (first, last) in enumerate(spans):
        for b in range(first, last):
            store(n, b - low).wait()


def turn(blocks, spans):
    _, rows, window = blocks.shape
    count = max(last for _, last in spans) - min(first for first, _ in spans)
    hbm = pl.BlockSpec(memory_space=pltpu.HBM)
    return pl.pallas_call(
        functools.partial(turn_kernel, spans),
        out_shape=[
            jax.ShapeDtypeStruct((last - first, window, rows), jnp.float32)
            for first, last in spans
        ],
        in_specs=[hbm],
        out_specs=[hbm] * len(spans),
        scratch_shapes=[
            pltpu.VMEM((count, rows, window), jnp.float32),
            pltpu.VMEM((count, window, rows), jnp.float32),
            pltpu.SemaphoreType.DMA((count,)),
            pltpu.SemaphoreType.DMA((len(spans), count)),
        ],
        compiler_params=pltpu.CompilerParams(vmem_limit_bytes=WHOLE_VMEM),
        cost_estimate=pl.CostEstimate(
            flops=10**9, bytes_accessed=2 * count * rows * window * 4, transcendentals=0
        ),
    )(blocks)


def gram_kernel(place, blocks, other, kept, sent, q, v, gram, q_sems, v_sems):
    count = blocks.shape[0]

    def fetch(b):
        return (
            pltpu.make_async_copy(blocks.at[b], q.at[b], q_sems.at[b]),
            pltpu.make_async_copy(other.at[b], v.at[b], v_sems.at[b]),
        )

    for b in range(count):
        for copy in fetch(b):
            copy.start()
    gram[...] = jnp.zeros_like(gram)

    def step(n, _):
        for u in range(STEP):
            for copy in fetch(n * STEP + u):
                copy.wait()
        left, right = [], []
        for u in range(STEP):
            b = n * STEP + u
            high, low = split(q[b].T)
            vh, vl = split(v[b])
            left += [high, high, low]
            right += [vh, vl, vh]
        gram[...] += jnp.dot(
            jnp.concatenate(left, axis=1),
            jnp.concatenate(right, axis=0),
            preferred_element_type=jnp.float32,
        )
        return 0

    lax.fori_loop(0, count // STEP, step, 0)
    half = kept.shape[0]
    core = place[0]
    kept[...] = gram[pl.ds(pl.multiple_of(core * half, half), half), :]
    sent[...] = gram[pl.ds(pl.multiple_of((1 - core) * half, half), half), :]


def local_gram(place, blocks, other):
    count, rows, window = blocks.shape
    hbm = pl.BlockSpec(memory_space=pltpu.HBM)
    return pl.pallas_call(
        gram_kernel,
        out_shape=[jax.ShapeDtypeStruct((window // N_CORE, window), jnp.float32)] * 2,
        in_specs=[pl.BlockSpec(memory_space=pltpu.SMEM), hbm, hbm],
        out_specs=[pl.BlockSpec(memory_space=pltpu.VMEM)] * 2,
        scratch_shapes=[pltpu.VMEM((count, rows, window), jnp.float32)] * 2
        + [pltpu.VMEM((window, window), jnp.float32)]
        + [pltpu.SemaphoreType.DMA((count,))] * 2,
        compiler_params=pltpu.CompilerParams(vmem_limit_bytes=WHOLE_VMEM),
        cost_estimate=pl.CostEstimate(
            flops=6 * count * rows * window * window, bytes_accessed=2**23, transcendentals=0
        ),
        name="gram",
    )(place, blocks, other)


def weigh(place, mine, other, factor, sh, sl):
    half = mine.shape[0]
    core, x, z = place[0], place[1], place[2]
    size = half // (N_X * N_Z)
    for index, ref in enumerate((mine, other)):
        start = jnp.where(core == index, 0, half)
        for i in range(N_X):
            for j in range(N_Z):
                at = start + (lax.rem(x + N_X - i, N_X) * N_Z + lax.rem(z + N_Z - j, N_Z)) * size
                rows = pl.ds(pl.multiple_of(at, size), size)
                part_of = ref[(i * N_Z + j) * size : (i * N_Z + j + 1) * size, :]
                sh[rows, :], sl[rows, :] = split(factor[rows, :] * part_of)


def make_adjoints(fetch, q, sh, sl, adjoints, keep):
    def some(n, _):
        for u in range(STEP):
            fetch(n * STEP + u).wait()
        highs, lows = zip(*[split(q[n * STEP + u]) for u in range(STEP)])
        tall = STEP * BS
        first = jnp.dot(
            jnp.concatenate(highs + lows, axis=0), sh[...], preferred_element_type=jnp.float32
        )
        second = jnp.dot(
            jnp.concatenate(highs, axis=0), sl[...], preferred_element_type=jnp.float32
        )
        high, low = split(first[:tall] + (first[tall:] + second))
        for u in range(STEP):
            i = n * STEP + u
            adjoints[i, :BS, :] = high[u * BS : (u + 1) * BS]
            adjoints[i, BS:, :] = low[u * BS : (u + 1) * BS]
        for u in range(STEP):
            keep(n * STEP + u).start()
        return 0

    lax.fori_loop(0, q.shape[0] // STEP, some, 0)


def pair_kernel(counts, group, bounds, keys, *refs):
    n_src, n_blk = len(counts), sum(counts)
    if group == 0:
        place, blocks, mine, other, factor = refs[:5]
        sources = refs[5 : 5 + n_src]
        out, kept_adjoints, adjoints, fetched, stage, sems, fetch_sems = refs[5 + n_src : 12 + n_src]
        q, sh, sl, q_sems, keep_sems = refs[12 + n_src :]
        n_rows = blocks.shape[0]

        def fetch(i):
            return pltpu.make_async_copy(blocks.at[i], q.at[i], q_sems.at[i])

        def keep(i):
            return pltpu.make_async_copy(adjoints.at[i], kept_adjoints.at[i], keep_sems.at[i])

        for i in range(n_rows):
            fetch(i).start()
    else:
        given_adjoints = refs[0]
        sources = refs[1 : 1 + n_src]
        out, adjoints, fetched, stage, sems, fetch_sems, adjoint_sem = refs[2 + n_src :]
        adjoint_copy = pltpu.make_async_copy(given_adjoints, adjoints, adjoint_sem)
    pieces = [(source, b) for source, count in zip(sources, counts) for b in range(count)]
    for n, (source, b) in enumerate(pieces):
        pltpu.make_async_copy(source.at[b], fetched.at[n], fetch_sems.at[n]).start()
    if group == 0:
        weigh(place, mine, other, factor, sh, sl)
        make_adjoints(fetch, q, sh, sl, adjoints, keep)
    else:
        adjoint_copy.start()

    def arrive(n, _):
        pltpu.make_async_copy(sources[0].at[0], fetched.at[n], fetch_sems.at[n]).wait()
        return 0

    lax.fori_loop(0, n_blk, arrive, 0)
    if group:
        adjoint_copy.wait()
    first, last = bounds[group], bounds[group + 1]
    origin = bounds[group + 8]
    total = last - first

    def copy_out(slot, target):
        return pltpu.make_async_copy(stage.at[slot], out.at[target], sems.at[slot])

    def some(step, _):
        at = step * UNROLL
        products = []
        names = [keys[first + at + u] for u in range(UNROLL)]
        for one, two in zip(names[::2], names[1::2]):
            i = (jnp.maximum(one, 0) >> 4) & 15
            b1 = jnp.maximum((one >> 8) - origin, 0)
            b2 = jnp.maximum((two >> 8) - origin, 0)
            rows = adjoints[i]
            h1, l1 = split(fetched[b1])
            h2, l2 = split(fetched[b2])
            by_high = jnp.dot(
                rows,
                jnp.concatenate([h1, h2], axis=1),
                preferred_element_type=jnp.float32,
            )
            by_low = jnp.dot(
                rows[:BS],
                jnp.concatenate([l1, l2], axis=1),
                preferred_element_type=jnp.float32,
            )
            product = by_high[:BS] + (by_high[BS:] + by_low)
            products += [product[:, :BS], product[:, BS:]]
        for u in range(UNROLL):
            slot = lax.rem(at + u, STAGES)
            before = keys[jnp.maximum(first + at + u - STAGES, 0)]

            @pl.when((at + u >= STAGES) & (before >= 0))
            def _():
                copy_out(slot, 0).wait()

            stage[slot] = products[u]

            @pl.when(names[u] >= 0)
            def _():
                copy_out(slot, ((names[u] >> 4) & 15) * 12 + (names[u] & 15)).start()

        return 0

    steps = lax.div(total, UNROLL)
    lax.fori_loop(0, steps, some, 0)
    for s in range(STAGES):
        at = total - STAGES + s

        @pl.when((at >= 0) & (keys[jnp.maximum(first + at, 0)] >= 0))
        def _():
            copy_out(lax.rem(at, STAGES), 0).wait()

    if group == 0:
        for i in range(n_rows):
            keep(i).wait()


def pair_call(group, bounds, keys, sources, out, shape, adjoints, inputs):
    counts = tuple(s.shape[0] for s in sources)
    n_blk = sum(counts)
    window = sources[0].shape[1]
    rows = inputs[1].shape[0]
    smem = pl.BlockSpec(memory_space=pltpu.SMEM)
    vmem = pl.BlockSpec(memory_space=pltpu.VMEM)
    hbm = pl.BlockSpec(memory_space=pltpu.HBM)
    out_shape = [jax.ShapeDtypeStruct(shape, jnp.float32)]
    scratch = [
        pltpu.VMEM((rows, 2 * BS, window), jnp.bfloat16),
        pltpu.VMEM((n_blk, window, BS), jnp.float32),
        pltpu.VMEM((STAGES, BS, BS), jnp.float32),
        pltpu.SemaphoreType.DMA((STAGES,)),
        pltpu.SemaphoreType.DMA((n_blk,)),
    ]
    flops = n_blk * 16 * BS * BS * window
    if group == 0:
        operands = [bounds, keys, *inputs, *sources]
        specs = [smem] * 3 + [hbm] + [vmem] * 3 + [hbm] * len(sources)
        out_shape.append(jax.ShapeDtypeStruct((rows, 2 * BS, window), jnp.bfloat16))
        scratch += [
            pltpu.VMEM((rows, BS, window), jnp.float32),
            pltpu.VMEM((window, window), jnp.bfloat16),
            pltpu.VMEM((window, window), jnp.bfloat16),
            pltpu.SemaphoreType.DMA((rows,)),
            pltpu.SemaphoreType.DMA((rows,)),
        ]
        aliases = {}
    else:
        operands = [bounds, keys, adjoints, *sources, out]
        specs = [smem] * 2 + [hbm] * (len(sources) + 2)
        scratch += [pltpu.SemaphoreType.DMA]
        aliases = {len(operands) - 1: 0}
    results = pl.pallas_call(
        functools.partial(pair_kernel, counts, group),
        out_shape=out_shape,
        in_specs=specs,
        out_specs=[hbm] * len(out_shape),
        scratch_shapes=scratch,
        input_output_aliases=aliases,
        compiler_params=pltpu.CompilerParams(
            vmem_limit_bytes=(32, 18, 14)[group] * 2**20
        ),
        cost_estimate=pl.CostEstimate(
            flops=flops, bytes_accessed=8 * 2**20, transcendentals=0
        ),
    )(*operands)
    return results if group == 0 else (results[0], adjoints)


def body(eig_vectors, vec_cotangent, levels, order, neighbours):
    highest = lax.Precision.HIGHEST
    window = eig_vectors.shape[1]
    local_rows = eig_vectors.shape[0]
    blk_count = local_rows // BS
    n_nbr = neighbours.shape[1]
    my_row, my_sub = lax.axis_index("row"), lax.axis_index("sub")
    core, x, z = my_row % N_CORE, (my_row // N_CORE) % N_X, my_row // (N_CORE * N_X)
    blocks = eig_vectors.reshape(blk_count, BS, window)

    def spans_of(sizes):
        return [(sum(sizes[:n]), sum(sizes[: n + 1])) for n in range(len(sizes))]

    place = jnp.stack([core, x, z]).astype(jnp.int32)
    sub_spans, row_spans = spans_of(SUB_PIECES), spans_of(ROW_PIECES)
    start = turn(blocks, [sub_spans[0], row_spans[0]])
    kept_gram, sent_gram = local_gram(
        place, blocks, vec_cotangent.reshape(blk_count, BS, window)
    )
    rest = list(turn(blocks, sub_spans[1:] + row_spans[1:]))
    sub_own = [start[0]] + rest[: len(SUB_PIECES) - 1]
    row_own = [start[1]] + rest[len(SUB_PIECES) - 1 :]
    sub_low = [lax.ppermute(t, "sub", ring(N_SUB, 1)) for t in sub_own]
    sub_high = [lax.ppermute(t, "sub", ring(N_SUB, -1)) for t in sub_own]
    near = [lax.ppermute(t, "row", CORE_SWAP) for t in row_own]
    far = [lax.ppermute(t, "row", PASS_ON) for t in near]

    half = window // N_CORE
    total = kept_gram + lax.ppermute(sent_gram, "row", CORE_SWAP)
    quarter = half // N_X
    mine = part(total, x, quarter)
    for s in range(1, N_X):
        mine += lax.ppermute(part(total, (x + s) % N_X, quarter), "row", row_shift(0, s))
    piece = quarter // N_Z
    total = mine
    mine = part(total, z, piece)
    for s in range(1, N_Z):
        mine += lax.ppermute(part(total, (z + s) % N_Z, piece), "row", row_shift(s, 0))
    total = mine
    for s in range(1, N_SUB):
        total += lax.ppermute(mine, "sub", ring(N_SUB, s))
    total = gather_back(total, N_Z, lambda s: lax.ppermute(total, "row", row_shift(s, 0)))
    total = gather_back(total, N_X, lambda s: lax.ppermute(total, "row", row_shift(0, s)))
    other = lax.ppermute(total, "row", CORE_SWAP)
    columns = lax.broadcasted_iota(jnp.int32, (window, window), 1)
    picked = (order[:, None] == columns).astype(jnp.float32)
    energy = jnp.dot(picked, levels, precision=highest, preferred_element_type=jnp.float32)
    spread = energy[None, :] - energy[:, None]
    factor = spread / (spread * spread + broadening_sq)

    device = neighbours // blk_count
    local = neighbours % blk_count
    row_delta = (device // N_SUB - my_row + N_ROW) % N_ROW
    sub_delta = (device % N_SUB - my_sub + N_SUB) % N_SUB
    slot = jnp.where(sub_delta == 1, SUB_HIGH, jnp.where(sub_delta == N_SUB - 1, SUB_LOW, SELF))
    slot = jnp.where(row_delta == jnp.where(core == 0, 1, N_ROW - 1), NEAR, slot)
    slot = jnp.where(row_delta == jnp.where(core == 0, N_ROW - 1, 1), FAR, slot)
    own = [(SELF, low, array) for (low, _), array in zip(sub_spans, sub_own)]
    near = [(NEAR, low, array) for (low, _), array in zip(row_spans, near)]
    far = [(FAR, low, array) for (low, _), array in zip(row_spans, far)]
    sub = [
        [(SUB_LOW, low, below), (SUB_HIGH, low, above)]
        for (low, _), below, above in zip(sub_spans, sub_low, sub_high)
    ]
    groups = [
        own + near + [far[0]] + sub[0],
        [far[1]] + sub[1],
        far[2:] + sub[2],
    ]
    position = jnp.zeros_like(slot)
    base, origins = 0, []
    for group in groups:
        origins.append(base)
        for which, low, array in group:
            inside = (slot == which) & (local >= low) & (local < low + array.shape[0])
            position = jnp.where(inside, base + local - low, position)
            base += array.shape[0]
    group_of = sum((position >= o).astype(jnp.int32) for o in origins[1:])
    i_index = lax.broadcasted_iota(jnp.int32, position.shape, 0)
    k_index = lax.broadcasted_iota(jnp.int32, position.shape, 1)
    same = group_of[:, :, None] == group_of[:, None, :]
    before = k_index[:, None, :] < k_index[:, :, None]
    within = jnp.sum((same & before).astype(jnp.int32), axis=2)
    n_groups = len(groups)

    each = jnp.arange(n_groups)
    counts = jnp.sum((group_of[:, :, None] == each).astype(jnp.int32), axis=1)
    room = (counts + 1) // 2 * 2
    earlier = (jnp.arange(blk_count)[:, None] > jnp.arange(blk_count)[None, :]).astype(jnp.int32)
    row_start = jnp.sum(earlier[:, :, None] * room[None, :, :], axis=1)
    sizes = (jnp.sum(room, axis=0) + UNROLL - 1) // UNROLL * UNROLL
    starts = jnp.sum(jnp.where(each[:, None] > each[None, :], sizes[None, :], 0), axis=1)
    table = row_start + starts[None, :]
    place_of = within + jnp.sum(
        jnp.where(group_of[:, :, None] == each, table[:, None, :], 0), axis=2
    )
    key = (position * 256 + i_index * 16 + k_index).reshape(-1)
    n_places = (blk_count * (n_nbr + n_groups) // UNROLL + n_groups) * UNROLL
    places = lax.broadcasted_iota(jnp.int32, (n_places, key.shape[0]), 0)
    found = jnp.where(place_of.reshape(1, -1) == places, key[None, :] + 1, 0)
    keys = jnp.sum(found, axis=1) - 1
    ends = jnp.concatenate([starts, jnp.sum(sizes)[None]])
    bounds = jnp.concatenate(
        [ends, jnp.zeros((8 - n_groups - 1,), jnp.int32), jnp.array(origins, jnp.int32)]
    )

    out = adjoints = None
    shape = (blk_count * n_nbr, BS, BS)
    inputs = [place, blocks, total, other, factor]
    for index, group in enumerate(groups):
        arrays = [g[2] for g in group]
        out, adjoints = pair_call(index, bounds, keys, arrays, out, shape, adjoints, inputs)
    return out.reshape(blk_count, n_nbr, BS, BS)


def solution(mesh):
    in_specs = (P(("row", "sub"), None), P(("row", "sub"), None), P(), P(), P(("row", "sub"), None))
    out_specs = P(("row", "sub"), None, None, None)
    return jax.shard_map(body, mesh=mesh, in_specs=in_specs, out_specs=out_specs, check_vma=False)
```

```python
import functools

import jax
import jax.numpy as jnp
from jax import lax
from jax.experimental import pallas as pl
from jax.experimental.pallas import tpu as pltpu
from jax.sharding import PartitionSpec as P


BS = 128
broadening_sq = 0.0025

N_CORE, N_X, N_Z = 2, 4, 4
N_ROW, N_SUB = N_CORE * N_X * N_Z, 4

SUB_PIECES = (6, 8, 2)
ROW_PIECES = (4, 6, 4, 2)
STAGES, STEP = 32, 4
UNROLLS = (16, 8, 8)
WHOLE_VMEM = 62 * 2**20
SELF, NEAR, FAR, SUB_LOW, SUB_HIGH = range(5)


def row_shift(dz, dx):
    pairs = []
    for r in range(N_ROW):
        core, x, z = r % N_CORE, (r // N_CORE) % N_X, r // (N_CORE * N_X)
        target = (((z + dz) % N_Z) * N_X + (x + dx) % N_X) * N_CORE + core
        pairs.append((r, target))
    return pairs


CORE_SWAP = [(r, r ^ 1) for r in range(N_ROW)]


PASS_ON = [(r, (r + (-2 if r % 2 else 2)) % N_ROW) for r in range(N_ROW)]


def ring(count, step):
    return [(i, (i + step) % count) for i in range(count)]


def part(array, index, size):
    return lax.dynamic_slice_in_dim(array, index * size, size, axis=0)


def gather_back(mine, count, send):
    return jnp.concatenate([mine] + [send(step) for step in range(1, count)])


def split(value):
    high = value.astype(jnp.bfloat16)
    return high, (value - high.astype(jnp.float32)).astype(jnp.bfloat16)


def turn_kernel(spans, blocks, *refs):
    n_out = len(spans)
    outs = refs[:n_out]
    q, turned, q_sems, t_sems = refs[n_out:]
    low = min(first for first, _ in spans)
    count = q.shape[0]

    def fetch(b):
        return pltpu.make_async_copy(blocks.at[low + b], q.at[b], q_sems.at[b])

    def store(n, b):
        at = low + b - spans[n][0]
        return pltpu.make_async_copy(turned.at[b], outs[n].at[at], t_sems.at[n, b])

    for b in range(count):
        fetch(b).start()

    def step(b, _):
        fetch(b).wait()
        turned[b] = q[b].T
        for n, (first, last) in enumerate(spans):

            @pl.when((low + b >= first) & (low + b < last))
            def _(n=n):
                store(n, b).start()

        return 0

    lax.fori_loop(0, count, step, 0)
    for n, (first, last) in enumerate(spans):
        for b in range(first, last):
            store(n, b - low).wait()


def turn(blocks, spans):
    _, rows, window = blocks.shape
    count = max(last for _, last in spans) - min(first for first, _ in spans)
    hbm = pl.BlockSpec(memory_space=pltpu.HBM)
    return pl.pallas_call(
        functools.partial(turn_kernel, spans),
        out_shape=[
            jax.ShapeDtypeStruct((last - first, window, rows), jnp.float32)
            for first, last in spans
        ],
        in_specs=[hbm],
        out_specs=[hbm] * len(spans),
        scratch_shapes=[
            pltpu.VMEM((count, rows, window), jnp.float32),
            pltpu.VMEM((count, window, rows), jnp.float32),
            pltpu.SemaphoreType.DMA((count,)),
            pltpu.SemaphoreType.DMA((len(spans), count)),
        ],
        compiler_params=pltpu.CompilerParams(vmem_limit_bytes=WHOLE_VMEM),
        cost_estimate=pl.CostEstimate(
            flops=10**9, bytes_accessed=2 * count * rows * window * 4, transcendentals=0
        ),
    )(blocks)


def gram_kernel(place, blocks, other, kept, sent, q, v, gram, q_sems, v_sems):
    count = blocks.shape[0]

    def fetch(b):
        return (
            pltpu.make_async_copy(blocks.at[b], q.at[b], q_sems.at[b]),
            pltpu.make_async_copy(other.at[b], v.at[b], v_sems.at[b]),
        )

    for b in range(count):
        for copy in fetch(b):
            copy.start()
    gram[...] = jnp.zeros_like(gram)

    def step(n, _):
        for u in range(STEP):
            for copy in fetch(n * STEP + u):
                copy.wait()
        left, right = [], []
        for u in range(STEP):
            b = n * STEP + u
            high, low = split(q[b].T)
            vh, vl = split(v[b])
            left += [high, high, low]
            right += [vh, vl, vh]
        gram[...] += jnp.dot(
            jnp.concatenate(left, axis=1),
            jnp.concatenate(right, axis=0),
            preferred_element_type=jnp.float32,
        )
        return 0

    lax.fori_loop(0, count // STEP, step, 0)
    half = kept.shape[0]
    core = place[0]
    kept[...] = gram[pl.ds(pl.multiple_of(core * half, half), half), :]
    sent[...] = gram[pl.ds(pl.multiple_of((1 - core) * half, half), half), :]


def local_gram(place, blocks, other):
    count, rows, window = blocks.shape
    hbm = pl.BlockSpec(memory_space=pltpu.HBM)
    return pl.pallas_call(
        gram_kernel,
        out_shape=[jax.ShapeDtypeStruct((window // N_CORE, window), jnp.float32)] * 2,
        in_specs=[pl.BlockSpec(memory_space=pltpu.SMEM), hbm, hbm],
        out_specs=[pl.BlockSpec(memory_space=pltpu.VMEM)] * 2,
        scratch_shapes=[pltpu.VMEM((count, rows, window), jnp.float32)] * 2
        + [pltpu.VMEM((window, window), jnp.float32)]
        + [pltpu.SemaphoreType.DMA((count,))] * 2,
        compiler_params=pltpu.CompilerParams(vmem_limit_bytes=WHOLE_VMEM),
        cost_estimate=pl.CostEstimate(
            flops=6 * count * rows * window * window, bytes_accessed=2**23, transcendentals=0
        ),
        name="gram",
    )(place, blocks, other)


def weigh(place, mine, other, factor, sh, sl):
    half = mine.shape[0]
    core, x, z = place[0], place[1], place[2]
    size = half // (N_X * N_Z)
    for index, ref in enumerate((mine, other)):
        start = jnp.where(core == index, 0, half)
        for i in range(N_X):
            for j in range(N_Z):
                at = start + (lax.rem(x + N_X - i, N_X) * N_Z + lax.rem(z + N_Z - j, N_Z)) * size
                rows = pl.ds(pl.multiple_of(at, size), size)
                part_of = ref[(i * N_Z + j) * size : (i * N_Z + j + 1) * size, :]
                sh[rows, :], sl[rows, :] = split(factor[rows, :] * part_of)


def make_adjoints(fetch, q, sh, sl, adjoints, keep, turned):
    def some(n, _):
        for u in range(STEP):
            fetch(n * STEP + u).wait()
        for u in range(STEP):
            turned[n * STEP + u] = q[n * STEP + u].T
        highs, lows = zip(*[split(q[n * STEP + u]) for u in range(STEP)])
        tall = STEP * BS
        first = jnp.dot(
            jnp.concatenate(highs + lows, axis=0), sh[...], preferred_element_type=jnp.float32
        )
        second = jnp.dot(
            jnp.concatenate(highs, axis=0), sl[...], preferred_element_type=jnp.float32
        )
        high, low = split(first[:tall] + (first[tall:] + second))
        for u in range(STEP):
            i = n * STEP + u
            adjoints[i, :BS, :] = high[u * BS : (u + 1) * BS]
            adjoints[i, BS:, :] = low[u * BS : (u + 1) * BS]
        for u in range(STEP):
            keep(n * STEP + u).start()
        return 0

    lax.fori_loop(0, q.shape[0] // STEP, some, 0)


def pair_kernel(counts, group, bounds, keys, *refs):
    n_src = len(counts)
    n_own = 0
    if group == 0:
        place, blocks, mine, other, factor = refs[:5]
        n_own = blocks.shape[0]
        sources = refs[5 : 5 + n_src]
        out, kept_adjoints, adjoints, fetched, stage, sems, fetch_sems = refs[5 + n_src : 12 + n_src]
        q, sh, sl, q_sems, keep_sems = refs[12 + n_src :]
        n_rows = blocks.shape[0]

        def fetch(i):
            return pltpu.make_async_copy(blocks.at[i], q.at[i], q_sems.at[i])

        def keep(i):
            return pltpu.make_async_copy(adjoints.at[i], kept_adjoints.at[i], keep_sems.at[i])

        for i in range(n_rows):
            fetch(i).start()
    else:
        given_adjoints = refs[0]
        sources = refs[1 : 1 + n_src]
        out, adjoints, fetched, stage, sems, fetch_sems, adjoint_sem = refs[2 + n_src :]
        adjoint_copy = pltpu.make_async_copy(given_adjoints, adjoints, adjoint_sem)
    n_blk = n_own + sum(counts)
    pieces = [(source, b) for source, count in zip(sources, counts) for b in range(count)]
    for n, (source, b) in enumerate(pieces, n_own):
        pltpu.make_async_copy(source.at[b], fetched.at[n], fetch_sems.at[n]).start()
    if group == 0:
        weigh(place, mine, other, factor, sh, sl)
        make_adjoints(fetch, q, sh, sl, adjoints, keep, fetched)
    else:
        adjoint_copy.start()

    def arrive(n, _):
        pltpu.make_async_copy(sources[0].at[0], fetched.at[n], fetch_sems.at[n]).wait()
        return 0

    lax.fori_loop(n_own, n_blk, arrive, 0)
    if group:
        adjoint_copy.wait()
    first, last = bounds[group], bounds[group + 1]
    unroll = UNROLLS[group]
    origin = bounds[group + 8]
    total = last - first

    def copy_out(slot, target):
        return pltpu.make_async_copy(stage.at[slot], out.at[target], sems.at[slot])

    def some(step, _):
        at = step * unroll
        products = []
        names = [keys[first + at + u] for u in range(unroll)]
        for one, two in zip(names[::2], names[1::2]):
            i = (jnp.maximum(one, 0) >> 4) & 15
            b1 = jnp.maximum((one >> 8) - origin, 0)
            b2 = jnp.maximum((two >> 8) - origin, 0)
            rows = adjoints[i]
            h1, l1 = split(fetched[b1])
            h2, l2 = split(fetched[b2])
            by_high = jnp.dot(
                rows,
                jnp.concatenate([h1, h2], axis=1),
                preferred_element_type=jnp.float32,
            )
            by_low = jnp.dot(
                rows[:BS],
                jnp.concatenate([l1, l2], axis=1),
                preferred_element_type=jnp.float32,
            )
            product = by_high[:BS] + (by_high[BS:] + by_low)
            products += [product[:, :BS], product[:, BS:]]
        for u in range(unroll):
            slot = lax.rem(at + u, STAGES)
            before = keys[jnp.maximum(first + at + u - STAGES, 0)]

            @pl.when((at + u >= STAGES) & (before >= 0))
            def _():
                copy_out(slot, 0).wait()

            stage[slot] = products[u]

            @pl.when(names[u] >= 0)
            def _():
                copy_out(slot, ((names[u] >> 4) & 15) * 12 + (names[u] & 15)).start()

        return 0

    steps = lax.div(total, unroll)
    lax.fori_loop(0, steps, some, 0)
    for s in range(STAGES):
        at = total - STAGES + s

        @pl.when((at >= 0) & (keys[jnp.maximum(first + at, 0)] >= 0))
        def _():
            copy_out(lax.rem(at, STAGES), 0).wait()

    if group == 0:
        for i in range(n_rows):
            keep(i).wait()


def pair_call(group, bounds, keys, sources, out, shape, adjoints, inputs):
    counts = tuple(s.shape[0] for s in sources)
    window = sources[0].shape[1]
    rows = inputs[1].shape[0]
    n_blk = sum(counts) + (rows if group == 0 else 0)
    smem = pl.BlockSpec(memory_space=pltpu.SMEM)
    vmem = pl.BlockSpec(memory_space=pltpu.VMEM)
    hbm = pl.BlockSpec(memory_space=pltpu.HBM)
    out_shape = [jax.ShapeDtypeStruct(shape, jnp.float32)]
    scratch = [
        pltpu.VMEM((rows, 2 * BS, window), jnp.bfloat16),
        pltpu.VMEM((n_blk, window, BS), jnp.float32),
        pltpu.VMEM((STAGES, BS, BS), jnp.float32),
        pltpu.SemaphoreType.DMA((STAGES,)),
        pltpu.SemaphoreType.DMA((n_blk,)),
    ]
    flops = n_blk * 16 * BS * BS * window
    if group == 0:
        operands = [bounds, keys, *inputs, *sources]
        specs = [smem] * 3 + [hbm] + [vmem] * 3 + [hbm] * len(sources)
        out_shape.append(jax.ShapeDtypeStruct((rows, 2 * BS, window), jnp.bfloat16))
        scratch += [
            pltpu.VMEM((rows, BS, window), jnp.float32),
            pltpu.VMEM((window, window), jnp.bfloat16),
            pltpu.VMEM((window, window), jnp.bfloat16),
            pltpu.SemaphoreType.DMA((rows,)),
            pltpu.SemaphoreType.DMA((rows,)),
        ]
        aliases = {}
    else:
        operands = [bounds, keys, adjoints, *sources, out]
        specs = [smem] * 2 + [hbm] * (len(sources) + 2)
        scratch += [pltpu.SemaphoreType.DMA]
        aliases = {len(operands) - 1: 0}
    results = pl.pallas_call(
        functools.partial(pair_kernel, counts, group),
        out_shape=out_shape,
        in_specs=specs,
        out_specs=[hbm] * len(out_shape),
        scratch_shapes=scratch,
        input_output_aliases=aliases,
        compiler_params=pltpu.CompilerParams(
            vmem_limit_bytes=(34, 18, 14)[group] * 2**20
        ),
        cost_estimate=pl.CostEstimate(
            flops=flops, bytes_accessed=8 * 2**20, transcendentals=0
        ),
    )(*operands)
    return results if group == 0 else (results[0], adjoints)


def body(eig_vectors, vec_cotangent, levels, order, neighbours):
    highest = lax.Precision.HIGHEST
    window = eig_vectors.shape[1]
    local_rows = eig_vectors.shape[0]
    blk_count = local_rows // BS
    n_nbr = neighbours.shape[1]
    my_row, my_sub = lax.axis_index("row"), lax.axis_index("sub")
    core, x, z = my_row % N_CORE, (my_row // N_CORE) % N_X, my_row // (N_CORE * N_X)
    blocks = eig_vectors.reshape(blk_count, BS, window)

    def spans_of(sizes):
        return [(sum(sizes[:n]), sum(sizes[: n + 1])) for n in range(len(sizes))]

    place = jnp.stack([core, x, z]).astype(jnp.int32)
    sub_spans, row_spans = spans_of(SUB_PIECES), spans_of(ROW_PIECES)
    start = turn(blocks, [sub_spans[0], row_spans[0]])
    kept_gram, sent_gram = local_gram(
        place, blocks, vec_cotangent.reshape(blk_count, BS, window)
    )
    rest = list(turn(blocks, sub_spans[1:] + row_spans[1:]))
    sub_own = [start[0]] + rest[: len(SUB_PIECES) - 1]
    row_own = [start[1]] + rest[len(SUB_PIECES) - 1 :]
    sub_low = [lax.ppermute(t, "sub", ring(N_SUB, 1)) for t in sub_own]
    sub_high = [lax.ppermute(t, "sub", ring(N_SUB, -1)) for t in sub_own]
    near = [lax.ppermute(t, "row", CORE_SWAP) for t in row_own]
    far = [lax.ppermute(t, "row", PASS_ON) for t in near]

    half = window // N_CORE
    total = kept_gram + lax.ppermute(sent_gram, "row", CORE_SWAP)
    quarter = half // N_X
    mine = part(total, x, quarter)
    for s in range(1, N_X):
        mine += lax.ppermute(part(total, (x + s) % N_X, quarter), "row", row_shift(0, s))
    piece = quarter // N_Z
    total = mine
    mine = part(total, z, piece)
    for s in range(1, N_Z):
        mine += lax.ppermute(part(total, (z + s) % N_Z, piece), "row", row_shift(s, 0))
    total = mine
    for s in range(1, N_SUB):
        total += lax.ppermute(mine, "sub", ring(N_SUB, s))
    total = gather_back(total, N_Z, lambda s: lax.ppermute(total, "row", row_shift(s, 0)))
    total = gather_back(total, N_X, lambda s: lax.ppermute(total, "row", row_shift(0, s)))
    other = lax.ppermute(total, "row", CORE_SWAP)
    columns = lax.broadcasted_iota(jnp.int32, (window, window), 1)
    picked = (order[:, None] == columns).astype(jnp.float32)
    energy = jnp.dot(picked, levels, precision=highest, preferred_element_type=jnp.float32)
    spread = energy[None, :] - energy[:, None]
    factor = spread / (spread * spread + broadening_sq)

    device = neighbours // blk_count
    local = neighbours % blk_count
    row_delta = (device // N_SUB - my_row + N_ROW) % N_ROW
    sub_delta = (device % N_SUB - my_sub + N_SUB) % N_SUB
    slot = jnp.where(sub_delta == 1, SUB_HIGH, jnp.where(sub_delta == N_SUB - 1, SUB_LOW, SELF))
    slot = jnp.where(row_delta == jnp.where(core == 0, 1, N_ROW - 1), NEAR, slot)
    slot = jnp.where(row_delta == jnp.where(core == 0, N_ROW - 1, 1), FAR, slot)
    own = [(SELF, low, array) for (low, _), array in zip(sub_spans, sub_own)]
    near = [(NEAR, low, array) for (low, _), array in zip(row_spans, near)]
    far = [(FAR, low, array) for (low, _), array in zip(row_spans, far)]
    sub = [
        [(SUB_LOW, low, below), (SUB_HIGH, low, above)]
        for (low, _), below, above in zip(sub_spans, sub_low, sub_high)
    ]
    groups = [
        own + near + [far[0]] + sub[0],
        [far[1]] + sub[1],
        far[2:] + sub[2],
    ]
    position = jnp.zeros_like(slot)
    base, origins = 0, []
    for group in groups:
        origins.append(base)
        for which, low, array in group:
            inside = (slot == which) & (local >= low) & (local < low + array.shape[0])
            position = jnp.where(inside, base + local - low, position)
            base += array.shape[0]
    group_of = sum((position >= o).astype(jnp.int32) for o in origins[1:])
    i_index = lax.broadcasted_iota(jnp.int32, position.shape, 0)
    k_index = lax.broadcasted_iota(jnp.int32, position.shape, 1)
    same = group_of[:, :, None] == group_of[:, None, :]
    before = k_index[:, None, :] < k_index[:, :, None]
    within = jnp.sum((same & before).astype(jnp.int32), axis=2)
    n_groups = len(groups)

    each = jnp.arange(n_groups)
    counts = jnp.sum((group_of[:, :, None] == each).astype(jnp.int32), axis=1)
    room = (counts + 1) // 2 * 2
    earlier = (jnp.arange(blk_count)[:, None] > jnp.arange(blk_count)[None, :]).astype(jnp.int32)
    row_start = jnp.sum(earlier[:, :, None] * room[None, :, :], axis=1)
    unrolls = jnp.array(UNROLLS, jnp.int32)
    sizes = (jnp.sum(room, axis=0) + unrolls - 1) // unrolls * unrolls
    starts = jnp.sum(jnp.where(each[:, None] > each[None, :], sizes[None, :], 0), axis=1)
    table = row_start + starts[None, :]
    place_of = within + jnp.sum(
        jnp.where(group_of[:, :, None] == each, table[:, None, :], 0), axis=2
    )
    key = (position * 256 + i_index * 16 + k_index).reshape(-1)
    n_places = blk_count * (n_nbr + n_groups) + sum(UNROLLS)
    places = lax.broadcasted_iota(jnp.int32, (n_places, key.shape[0]), 0)
    found = jnp.where(place_of.reshape(1, -1) == places, key[None, :] + 1, 0)
    keys = jnp.sum(found, axis=1) - 1
    ends = jnp.concatenate([starts, jnp.sum(sizes)[None]])
    bounds = jnp.concatenate(
        [ends, jnp.zeros((8 - n_groups - 1,), jnp.int32), jnp.array(origins, jnp.int32)]
    )

    out = adjoints = None
    shape = (blk_count * n_nbr, BS, BS)
    inputs = [place, blocks, total, other, factor]
    for index, group in enumerate(groups):
        arrays = [array for slot_of, _, array in group if slot_of != SELF]
        out, adjoints = pair_call(index, bounds, keys, arrays, out, shape, adjoints, inputs)
    return out.reshape(blk_count, n_nbr, BS, BS)


def solution(mesh):
    in_specs = (P(("row", "sub"), None), P(("row", "sub"), None), P(), P(), P(("row", "sub"), None))
    out_specs = P(("row", "sub"), None, None, None)
    return jax.shard_map(body, mesh=mesh, in_specs=in_specs, out_specs=out_specs, check_vma=False)
```
